32 devices in a mesh: node: 8 (over y, x, core), local: 4 (over z).
Axes of the slice: x: 2, y: 2, z: 4, core: 2. Of those that a mesh axis runs over, the one named last changes fastest.
Arguments:
- vit_tiles: bfloat16 [8, 4, 128, 12800], P('node', 'local'), may hold values from -6 to 6
- tile_counts: int32 [8, 1], P('node'), may hold values from 1 to 2
- block_of_piece: int32 [8, 2], P('node'), may hold values from 0 to 7, as said below
- segment_ids: int32 [8, 8, 256], P('node', None, 'local'), may hold values from 0 to 15, as said below
- text_rows: bfloat16 [8, 8, 256, 3584], P('node', None, 'local'), may hold values from -6 to 6
- cotangent: bfloat16 [8, 8, 256, 512], P('node', None, 'local'), may hold values from -6 to 6
- proj_weight: bfloat16 [12800, 3584], P('local', 'node'), may hold values from -0.0546875 to 0.0546875
- proj_bias: float32 [3584], replicated, may hold values from -3 to 3
- out_weight: bfloat16 [3584, 3584], P(None, 'local'), may hold values from -0.09375 to 0.09375
- out_bias: float32 [3584], replicated, may hold values from -3 to 3
- ln_gain: float32 [12800], replicated, may hold values from 0.25 to 1.75
- ln_bias: float32 [12800], replicated, may hold values from -2 to 2
- norm_gain: float32 [3584], replicated, may hold values from 0.25 to 1.75
- v_weight: bfloat16 [3584, 512], P(('node', 'local')), may hold values from -0.09375 to 0.09375
Outputs:
- hidden_grad: bfloat16 [8, 8, 256, 3584], P('node', None, 'local')
- value_weight_grad: float32 [3584, 512], P(('node', 'local'))
- value_bias_grad: float32 [512], replicated
- norm_gain_grad: float32 [3584], replicated
The draws below stay inside these ranges and needn't reach their ends.
Inputs may be any that keep to these rules, and one draw needn't show every extreme that they name: `block_of_piece`: within one sequence the entries are distinct. `segment_ids`: along each sequence, read block by block, the ids never fall; every sequence has exactly 16 documents.
All inputs are finite; a program needn't handle non-finite values.
Results may differ from the reference program's by a relative error of at most 0.017.
Values may be sent and summed in bfloat16 or wider, within the bound.
A program may use at most 128 MiB of HBM per device.

```python
import jax
import jax.numpy as jnp
from jax import lax

VW = 12800
D = 3584
KV = 512
TILE_TOK = 256
SLOTS = 2
BLOCKS = 8
DOCS = 16
HALF = 128
PIECES = 2
IMAGES = 1
N_NODE = 8
N_LOCAL = 4


def draw_block_of_piece(key, part):
    node_keys = jax.random.split(jax.random.fold_in(key, 11), N_NODE)

    def one_node(node_key):
        return jax.random.permutation(node_key, BLOCKS)[:PIECES].astype(jnp.int32)
    return jax.vmap(one_node)(node_keys)


def draw_segment_ids(key, part):
    node_keys = jax.random.split(jax.random.fold_in(key, 23), N_NODE)
    length = BLOCKS * TILE_TOK

    def one_node(node_key):
        starts = jax.random.permutation(node_key, length - 1)[:DOCS - 1] + 1
        boundary = jnp.zeros((length,), jnp.int32).at[starts].set(1)
        return jnp.cumsum(boundary).astype(jnp.int32).reshape(BLOCKS, TILE_TOK)
    return jax.vmap(one_node)(node_keys)


def set_ends(result, stream_key, smallest, top_value):
    shape = result.shape
    place = [jax.random.randint(jax.random.fold_in(stream_key, axis), (), 0, shape[axis]) for axis in range(len(shape))]
    result = result.at[tuple(place)].set(smallest)
    longest = shape.index(max(shape))
    place[longest] = (place[longest] + 1) % shape[longest]
    return result.at[tuple(place)].set(top_value)


def block_levels(stream_key, shape, cuts, smallest, high):
    factor_of, own = 1.0, jax.random.fold_in(stream_key, 6)
    for dim, parts in cuts:
        steps = jnp.exp(jax.random.uniform(jax.random.fold_in(own, dim), (parts,), jnp.float32, smallest / len(cuts), high / len(cuts)))
        factor_of = factor_of * jnp.repeat(steps, shape[dim] // parts).reshape([-1 if axis == dim else 1 for axis in range(len(shape))])
    return factor_of


def scatter_about(stream_key, dims, scale, most, shards=(), kind=jnp.bfloat16):
    result = jax.random.normal(stream_key, dims, jnp.float32) * scale
    if len(shards) > 0:
        result = block_levels(stream_key, dims, shards, -0.22, 0.18) * result
    return jnp.clip(result, min=-most, max=most).astype(kind)


def setup_inputs(seed: int = 0) -> dict:
    streams_of = jax.random.split(jax.random.key(seed), 15)
    return {
        "vit_tiles": scatter_about(streams_of[0], (N_NODE, N_LOCAL, HALF, VW), 1.0, 6.0, ((0, 8), (1, 4))),
        "tile_counts": set_ends(jax.random.randint(streams_of[1], (N_NODE, IMAGES), 1, SLOTS + 1), jax.random.fold_in(streams_of[1], 1), 1, SLOTS).astype(jnp.int32),
        "block_of_piece": draw_block_of_piece(jax.random.fold_in(streams_of[14], 71), 0),
        "segment_ids": draw_segment_ids(jax.random.fold_in(streams_of[14], 71), 0),
        "text_rows": scatter_about(streams_of[4], (N_NODE, BLOCKS, TILE_TOK, D), 1.0, 6.0, ((0, 8), (2, 4))),
        "cotangent": scatter_about(streams_of[5], (N_NODE, BLOCKS, TILE_TOK, KV), 1.0, 6.0, ((0, 8), (2, 4))),
        "proj_weight": scatter_about(streams_of[6], (VW, D), VW ** -0.5, 0.0546875, ((0, 4), (1, 8))),
        "proj_bias": scatter_about(streams_of[7], (D,), 0.5, 3.0, (), jnp.float32),
        "out_weight": scatter_about(streams_of[8], (D, D), D ** -0.5, 0.09375, ((1, 4),)),
        "out_bias": scatter_about(streams_of[9], (D,), 0.5, 3.0, (), jnp.float32),
        "ln_gain": jnp.clip(1.0 + 0.15 * jax.random.normal(streams_of[10], (VW,), jnp.float32), 0.25, 1.75),
        "ln_bias": scatter_about(streams_of[11], (VW,), 0.4, 2.0, (), jnp.float32),
        "norm_gain": jnp.clip(1.0 + 0.15 * jax.random.normal(streams_of[12], (D,), jnp.float32), 0.25, 1.75),
        "v_weight": scatter_about(streams_of[13], (D, KV), D ** -0.5, 0.09375, ((0, 32),)),
    }


def layer_norm(vit_rows, scale_vec, shift_vec):
    values = vit_rows.astype(jnp.float32)
    average = lax.optimization_barrier(jnp.mean(values, -1, keepdims=True))
    centred = values - average
    variance = lax.optimization_barrier(jnp.mean(centred * centred, -1, keepdims=True))
    return (centred * lax.rsqrt(variance + 1e-05) * scale_vec + shift_vec).astype(jnp.bfloat16)

def reference(vit_tiles, tile_counts, block_of_piece, segment_ids, text_rows, cotangent, proj_weight, proj_bias, out_weight, out_bias, ln_gain, ln_bias, norm_gain, v_weight):
    piece_total = N_LOCAL // 2
    slice_width = VW // N_LOCAL
    half_rows = TILE_TOK // 2
    run_rows = TILE_TOK // (2 * N_LOCAL)

    def one_sequence(sequence):
        normed = layer_norm(vit_tiles[sequence].reshape(N_LOCAL * half_rows, VW), ln_gain, ln_bias)
        preact = jnp.zeros((N_LOCAL * half_rows, D), jnp.float32)
        for slice_index in range(N_LOCAL):
            lower = slice_index * slice_width
            term = jnp.dot(normed[:, lower:lower + slice_width], proj_weight[lower:lower + slice_width], preferred_element_type=jnp.float32)
            term = lax.optimization_barrier(term.astype(jnp.bfloat16))
            preact = preact + term.astype(jnp.float32)
        middle = jax.nn.gelu(preact + proj_bias, approximate=False).astype(jnp.bfloat16)
        projected = (jnp.dot(middle, out_weight, preferred_element_type=jnp.float32) + out_bias).astype(jnp.bfloat16)
        projected = projected.reshape(piece_total, 2, N_LOCAL, run_rows, D).transpose(0, 2, 1, 3, 4).reshape(piece_total, TILE_TOK, D)
        filled = jnp.arange(piece_total, dtype=jnp.int32) % SLOTS < jnp.repeat(tile_counts[sequence], SLOTS)
        chosen = (block_of_piece[sequence][None, :] == jnp.arange(BLOCKS, dtype=jnp.int32)[:, None]) & filled[None, :]
        placed = jnp.einsum('bp,ptd->btd', chosen.astype(jnp.float32), projected.astype(jnp.float32))
        is_image = lax.optimization_barrier(jnp.sum(chosen.astype(jnp.int32), 1)) > 0
        hidden = jnp.where(is_image[:, None, None], placed.astype(jnp.bfloat16), text_rows[sequence])
        doc_ids = segment_ids[sequence].reshape(-1)
        doc_sizes = lax.optimization_barrier(jnp.sum((doc_ids[:, None] == jnp.arange(DOCS, dtype=jnp.int32)[None, :]).astype(jnp.float32), 0))
        doc_weight = BLOCKS * TILE_TOK / (DOCS * doc_sizes)
        token_weight = doc_weight[doc_ids]
        value_grad = (cotangent[sequence].reshape(-1, KV).astype(jnp.float32) * token_weight[:, None]).astype(jnp.bfloat16)
        hidden_f = hidden.reshape(-1, D).astype(jnp.float32)
        inv_rms = lax.rsqrt(lax.optimization_barrier(jnp.mean(hidden_f * hidden_f, -1, keepdims=True)) + 1e-06)
        normed_input = (hidden_f * inv_rms * norm_gain).astype(jnp.bfloat16)
        grad_normed = lax.dot_general(value_grad, v_weight, (((1,), (1,)), ((), ())), preferred_element_type=jnp.float32)
        gain_part = lax.optimization_barrier(jnp.sum(grad_normed * hidden_f * inv_rms, 0))
        scaled = grad_normed * norm_gain
        grad_hidden = inv_rms * scaled - hidden_f * (inv_rms * inv_rms * inv_rms) * lax.optimization_barrier(jnp.mean(scaled * hidden_f, -1, keepdims=True))
        weight_part = lax.dot_general(normed_input, value_grad, (((0,), (0,)), ((), ())), preferred_element_type=jnp.float32)
        bias_part = lax.optimization_barrier(jnp.sum(value_grad.astype(jnp.float32), 0))
        return (grad_hidden.astype(jnp.bfloat16).reshape(BLOCKS, TILE_TOK, D), weight_part, bias_part, gain_part)
    grad_hidden, weight_parts, bias_parts, gain_parts = lax.map(one_sequence, jnp.arange(N_NODE, dtype=jnp.int32))
    return (grad_hidden, lax.optimization_barrier(jnp.sum(weight_parts, 0)) / N_NODE, lax.optimization_barrier(jnp.sum(bias_parts, 0)) / N_NODE, lax.optimization_barrier(jnp.sum(gain_parts, 0)) / N_NODE)
```

```python
import jax
import jax.numpy as jnp
from jax import lax
from jax.experimental import pallas as pl
from jax.experimental.pallas import tpu as pltpu
from jax.sharding import PartitionSpec as P

SLOTS = 2
DOCS = 16
CHUNKS = 2


def tail_kernel(
    piece_ref,
    text_ref,
    arrived_ref,
    grad_ref,
    weight_ref,
    gain_ref,
    out_ref,
    normed_ref,
    part_ref,
    hidden_ref,
):
    block = pl.program_id(0)
    is_image = piece_ref[block] >= 0

    @pl.when(is_image)
    def _():
        hidden_ref[...] = arrived_ref[0].astype(jnp.float32)

    @pl.when(jnp.logical_not(is_image))
    def _():
        hidden_ref[...] = text_ref[0].astype(jnp.float32)

    hidden_f = hidden_ref[...]
    inv_rms = lax.rsqrt(jnp.mean(hidden_f * hidden_f, -1, keepdims=True) + 1e-06)
    gain = gain_ref[...]
    unit = hidden_f * inv_rms
    normed_ref[0] = (unit * gain).astype(jnp.bfloat16)
    grad_normed = lax.dot_general(
        grad_ref[0], weight_ref[...], (((1,), (1,)), ((), ())), preferred_element_type=jnp.float32
    )
    part = jnp.sum(grad_normed * unit, 0, keepdims=True)

    @pl.when(block == 0)
    def _():
        part_ref[...] = part

    @pl.when(block > 0)
    def _():
        part_ref[...] += part

    scaled = grad_normed * gain
    hidden_f = hidden_ref[...]
    moment = jnp.mean(scaled * hidden_f, -1, keepdims=True)
    out_ref[0] = (
        inv_rms * scaled - hidden_f * (inv_rms * inv_rms * inv_rms * moment)
    ).astype(jnp.bfloat16)


def tail(piece_of_block, text, arrived, value_grad, v_full, norm_gain):
    blocks, rows, width = text.shape
    values = value_grad.shape[2]
    row_block = pl.BlockSpec((1, rows, width), lambda b, piece: (b, 0, 0))
    return pl.pallas_call(
        tail_kernel,
        grid_spec=pltpu.PrefetchScalarGridSpec(
            num_scalar_prefetch=1,
            grid=(blocks,),
            in_specs=[
                row_block,
                pl.BlockSpec((1, rows, width), lambda b, piece: (jnp.maximum(piece[b], 0), 0, 0)),
                pl.BlockSpec((1, rows, values), lambda b, piece: (b, 0, 0)),
                pl.BlockSpec((width, values), lambda b, piece: (0, 0)),
                pl.BlockSpec((1, width), lambda b, piece: (0, 0)),
            ],
            out_specs=[row_block, row_block, pl.BlockSpec((1, width), lambda b, piece: (0, 0))],
            scratch_shapes=[pltpu.VMEM((rows, width), jnp.float32)],
        ),
        out_shape=[
            jax.ShapeDtypeStruct((blocks, rows, width), jnp.bfloat16),
            jax.ShapeDtypeStruct((blocks, rows, width), jnp.bfloat16),
            jax.ShapeDtypeStruct((1, width), jnp.float32),
        ],
        cost_estimate=pl.CostEstimate(
            flops=2 * blocks * rows * width * values,
            bytes_accessed=8 * blocks * rows * width,
            transcendentals=0,
        ),
    )(piece_of_block, text, arrived, value_grad, v_full, norm_gain[None, :])


def layer_norm(vit_rows, scale_vec, shift_vec):
    values = vit_rows.astype(jnp.float32)
    average = jnp.mean(values, -1, keepdims=True)
    centred = values - average
    variance = jnp.mean(centred * centred, -1, keepdims=True)
    return (centred * lax.rsqrt(variance + 1e-05) * scale_vec + shift_vec).astype(jnp.bfloat16)


def per_device(
    vit_tiles,
    tile_counts,
    block_of_piece,
    segment_ids,
    text_rows,
    cotangent,
    proj_weight,
    proj_bias,
    out_weight,
    out_bias,
    ln_gain,
    ln_bias,
    norm_gain,
    v_weight,
):
    local_count = lax.axis_size("local")
    node_count = lax.axis_size("node")
    own_index = lax.axis_index("local")
    blocks = text_rows.shape[1]
    share_rows = text_rows.shape[2]
    model_width = text_rows.shape[3]
    out_cols = out_weight.shape[1]
    normed = layer_norm(vit_tiles[0, 0], ln_gain, ln_bias)
    received = lax.all_to_all(normed, "local", split_axis=1, concat_axis=0, tiled=True)
    bias_cols = lax.dynamic_slice_in_dim(out_bias, own_index * out_cols, out_cols, 0)
    v_full = lax.all_gather(
        lax.all_gather(v_weight, "local", axis=0, tiled=True), "node", axis=0, tiled=True
    )
    doc_ids = segment_ids[0].reshape(-1)
    doc_hits = (doc_ids[:, None] == lax.iota(jnp.int32, DOCS)[None, :]).astype(jnp.float32)
    doc_sizes = lax.psum(jnp.sum(doc_hits, 0), "local")
    doc_weight = blocks * share_rows * local_count / (DOCS * doc_sizes)
    token_weight = jnp.dot(doc_hits, doc_weight, precision=lax.Precision.HIGHEST)
    value_grad = (
        cotangent[0].reshape(-1, cotangent.shape[3]).astype(jnp.float32) * token_weight[:, None]
    ).astype(jnp.bfloat16)
    bias_part = jnp.sum(value_grad.astype(jnp.float32), 0)
    width_each = proj_weight.shape[1] // CHUNKS
    bias_chunks = proj_bias.reshape(node_count, CHUNKS, width_each)
    out_chunks = out_weight.reshape(node_count, CHUNKS, width_each, out_cols)
    out_chunks = [out_chunks[:, c].reshape(-1, out_cols) for c in range(CHUNKS)]
    gathered = [
        lax.all_gather(
            proj_weight[:, c * width_each : (c + 1) * width_each], "node", axis=1, tiled=True
        )
        for c in range(CHUNKS)
    ]
    sums = []
    for c in range(CHUNKS):
        term = jnp.dot(received, gathered[c], preferred_element_type=jnp.float32)
        rounded = lax.optimization_barrier(term.astype(jnp.bfloat16))
        sums.append(lax.psum_scatter(rounded, "local", scatter_dimension=0, tiled=True))
    sums[0], value_grad, bias_part, out_chunks = lax.optimization_barrier(
        (sums[0], value_grad, bias_part, out_chunks)
    )
    projected = bias_cols
    for c in range(CHUNKS):
        middle = jax.nn.gelu(
            sums[c].astype(jnp.float32) + bias_chunks[:, c].reshape(-1), approximate=False
        ).astype(jnp.bfloat16)
        projected = projected + jnp.dot(
            lax.all_gather(middle, "local", axis=0, tiled=True),
            out_chunks[c],
            preferred_element_type=jnp.float32,
        )
    columns_out = projected.astype(jnp.bfloat16)
    run_rows = share_rows // 2
    columns_out = columns_out.reshape(local_count, local_count, run_rows, out_cols)
    arrived = lax.all_to_all(columns_out, "local", split_axis=1, concat_axis=3, tiled=True)
    piece_total = local_count // 2
    arrived = arrived.reshape(piece_total, share_rows, model_width)
    piece_ids = lax.iota(jnp.int32, piece_total)
    filled = piece_ids % SLOTS < jnp.repeat(tile_counts[0], SLOTS)
    chosen = (block_of_piece[0][None, :] == lax.iota(jnp.int32, blocks)[:, None]) & filled[None, :]
    piece_of_block = jnp.max(jnp.where(chosen, piece_ids[None, :], -1), 1).astype(jnp.int32)
    grad_hidden, normed_input, gain_part = tail(
        piece_of_block,
        text_rows[0],
        arrived,
        value_grad.reshape(blocks, share_rows, -1),
        v_full,
        norm_gain,
    )
    partial_sum = lax.psum_scatter(
        lax.dot_general(
            normed_input.reshape(-1, model_width),
            value_grad,
            (((0,), (0,)), ((), ())),
            preferred_element_type=jnp.float32,
        ).astype(jnp.bfloat16),
        "node",
        scatter_dimension=0,
        tiled=True,
    )
    grad_bias, grad_gain = lax.psum((bias_part, gain_part[0]), ("node", "local"))
    partial_sum, grad_bias, grad_gain = lax.optimization_barrier(
        (partial_sum, grad_bias, grad_gain)
    )
    grad_weight = lax.psum_scatter(partial_sum, "local", scatter_dimension=0, tiled=True).astype(
        jnp.float32
    )
    grad_hidden = grad_hidden[None]
    return (grad_hidden, grad_weight / node_count, grad_bias / node_count, grad_gain / node_count)


def solution(mesh):
    in_specs = (
        P("node", "local", None, None),
        P("node", None),
        P("node", None),
        P("node", None, "local"),
        P("node", None, "local", None),
        P("node", None, "local", None),
        P("local", "node"),
        P(),
        P(None, "local"),
        P(),
        P(),
        P(),
        P(),
        P(("node", "local"), None),
    )
    out_specs = (P("node", None, "local", None), P(("node", "local"), None), P(), P())
    return jax.shard_map(
        per_device, mesh=mesh, in_specs=in_specs, out_specs=out_specs, check_vma=False
    )
```
